16 devices in a mesh: dp: 2 (over y, z), ep: 8 (over x, core).
Axes of the slice: x: 4, y: 2, z: 1, core: 2. Of those that a mesh axis runs over, the one named last changes fastest.
The devices are a block of a 4x4x8 slice.
Arguments:
- x: bfloat16 [2, 8, 256, 4096], P('dp', 'ep'), parts along dimension 0
- expert: int32 [2, 8, 256, 8], P('dp', 'ep'), parts along dimension 0
- slot: int32 [2, 8, 256, 8], P('dp', 'ep'), parts along dimension 0
- gate: float32 [2, 8, 256, 8], P('dp', 'ep'), parts along dimension 0
- w_gate: bfloat16 [64, 4096, 1408], P('ep')
- w_up: bfloat16 [64, 4096, 1408], P('ep')
- w_down: bfloat16 [64, 1408, 4096], P('ep')
- s_gate: bfloat16 [4096, 1408], replicated
- s_up: bfloat16 [4096, 1408], replicated
- s_down: bfloat16 [1408, 4096], replicated
Outputs:
- y: bfloat16 [2, 8, 256, 4096], P('dp', 'ep'), parts along dimension 0
There are 2 independent parts. The reference program is written for one: setup_inputs(seed, part) draws one part's arguments, and reference() takes and returns one part's arrays. A program takes and returns all parts, laid end to end along the dimension named above; an argument that names none is the same for every part.
All inputs are finite; a program needn't handle non-finite values.
Results may differ from the reference program's by a relative error of at most 0.009.
Values are sent between devices in bfloat16 or wider.
A program may use at most 768 MiB of HBM per device.

```python
import jax
import jax.numpy as jnp

MEMBERS = 8
TOKENS = 256
D = 4096
FF = 1408
TOP = 8
EXPERTS = 64
SHARED_FF = 1408
SLOTS = 5 * TOKENS * TOP // (4 * EXPERTS)


def setup_inputs(seed: int = 0, part: int = 0) -> dict:
    own, k1, k2, k3, k4, k5, k6 = jax.random.split(jax.random.key(seed), 7)
    kx, ke, kl, kg = jax.random.split(jax.random.fold_in(own, part), 4)
    devices = (1, MEMBERS)
    place = jax.random.permutation(kl, jnp.arange(EXPERTS, dtype=jnp.uint32))
    slow = ((EXPERTS + (9 * place) % EXPERTS) << ((9 * place) // EXPERTS)) // EXPERTS
    wait = (jax.random.bits(ke, (*devices, TOKENS, EXPERTS), jnp.uint32) >> 10) * slow
    expert = jnp.argsort(wait, axis=-1)[..., :TOP].astype(jnp.int32)
    chosen = jax.nn.one_hot(expert, EXPERTS, dtype=jnp.int32)
    in_line = jnp.cumsum(chosen.reshape(*devices, TOKENS * TOP, EXPERTS), axis=2) - 1
    slot = jnp.sum(in_line.reshape(chosen.shape) * chosen, axis=-1)

    def one(key, rows, columns):
        return (jax.random.normal(key, (rows, columns), jnp.float32) * rows**-0.5).astype(jnp.bfloat16)

    def weights(key, rows, columns):
        return jax.lax.map(lambda k: one(k, rows, columns), jax.random.split(key, EXPERTS))

    return {
        "x": jax.random.normal(kx, (*devices, TOKENS, D), jnp.float32).astype(jnp.bfloat16),
        "expert": expert,
        "slot": slot,
        "gate": jax.nn.softmax(jax.random.normal(kg, expert.shape, jnp.float32)),
        "w_gate": weights(k1, D, FF),
        "w_up": weights(k2, D, FF),
        "w_down": weights(k3, FF, D),
        "s_gate": one(k4, D, SHARED_FF),
        "s_up": one(k5, D, SHARED_FF),
        "s_down": one(k6, SHARED_FF, D),
    }


def einsum(form, a, b):
    return jnp.einsum(form, a.astype(jnp.float32), b.astype(jnp.float32))


def for_all(x, s_gate, s_up, s_down):
    h = jax.nn.silu(einsum("...d,df->...f", x, s_gate)) * einsum("...d,df->...f", x, s_up)
    return einsum("...f,fd->...d", h.astype(jnp.bfloat16), s_down)


def reference(x, expert, slot, gate, w_gate, w_up, w_down, s_gate, s_up, s_down):
    to_expert = jax.nn.one_hot(expert, EXPERTS, dtype=jnp.bfloat16)
    to_slot = jax.nn.one_hot(slot, SLOTS, dtype=jnp.bfloat16)
    weighted = to_expert * gate[..., None].astype(jnp.bfloat16)
    dispatch = einsum("abtke,abtkc->abtec", to_expert, to_slot).astype(jnp.bfloat16)
    combine = einsum("abtke,abtkc->abtec", weighted, to_slot).astype(jnp.bfloat16)
    z = einsum("abtec,abtd->aebcd", dispatch, x).astype(jnp.bfloat16)
    h = jax.nn.silu(einsum("aebcd,edf->aebcf", z, w_gate))
    h = (h * einsum("aebcd,edf->aebcf", z, w_up)).astype(jnp.bfloat16)
    out = einsum("aebcf,efd->aebcd", h, w_down).astype(jnp.bfloat16)
    y = einsum("abtec,aebcd->abtd", combine, out)
    return (y + for_all(x, s_gate, s_up, s_down)).astype(jnp.bfloat16)
```

```python
import functools

import jax
import jax.numpy as jnp
from jax import lax
from jax.experimental import pallas as pl
from jax.experimental.pallas import tpu as pltpu
from jax.sharding import PartitionSpec as P

MESH = pl.DeviceIdType.MESH
BF, F32 = jnp.bfloat16, jnp.float32
ANY = pl.BlockSpec(memory_space=pl.ANY)
VM = pl.BlockSpec(memory_space=pltpu.VMEM)
W = 512
NT = 256


def dot(a, b):
    return jnp.dot(a, b, preferred_element_type=F32)


def remote(src, dst, send, recv, to):
    return pltpu.make_async_remote_copy(
        src_ref=src, dst_ref=dst, send_sem=send, recv_sem=recv,
        device_id={"ep": to}, device_id_type=MESH,
    )


def places():
    me = lax.axis_index("ep")
    chip, core = me // 2, me % 2
    at = lambda step: ((chip + step) % 4) * 2 + core
    return me, chip, core, chip * 2 + 1 - core, at(1), at(3), at(2)


def greet(n, me):
    barrier = pltpu.get_barrier_semaphore()
    for off in range(1, n):
        pl.semaphore_signal(barrier, inc=1, device_id={"ep": (me + off) % n}, device_id_type=MESH)
    pl.semaphore_wait(barrier, n - 1)


def project(n, slots, x, rt, sg, su, wg, wu, h_out, hs_out, rt_all,
            xg, oh, acc, wbuf, zf, z, hst, lsem, wsem, hsem, rts, rtr, own_s, own_r, fwd_s, fwd_r, par_s, par_r):
    per, _, ff = wg.shape
    T, D = x.shape
    half, rows, chunks = T // 2, n * slots, D // W
    me, chip, core, partner, right, left, opp = places()
    mine = per * slots

    def tile_copies(g, e, slot):
        return (
            pltpu.make_async_copy(wg.at[e, pl.ds(g * W, W), :], wbuf.at[slot, :, pl.ds(0, ff)], wsem.at[slot, 0]),
            pltpu.make_async_copy(wu.at[e, pl.ds(g * W, W), :], wbuf.at[slot, :, pl.ds(ff, ff)], wsem.at[slot, 1]),
        )

    def shared_copies(g, slot):
        return (
            pltpu.make_async_copy(sg.at[pl.ds(g * W, W), :], wbuf.at[slot, :, pl.ds(0, ff)], wsem.at[slot, 0]),
            pltpu.make_async_copy(su.at[pl.ds(g * W, W), :], wbuf.at[slot, :, pl.ds(ff, ff)], wsem.at[slot, 1]),
        )

    def fetch(t):
        slot = t % 3

        @pl.when(t < chunks)
        def _():
            for c in shared_copies(t, slot):
                c.start()

        @pl.when((t >= chunks) & (t < chunks + chunks * per))
        def _():
            for c in tile_copies((t - chunks) // per, (t - chunks) % per, slot):
                c.start()

    def arrived(t):
        for c in shared_copies(0, t % 3):
            c.wait()

    def local(k):
        return pltpu.make_async_copy(x.at[:, pl.ds(k * W, W)], xg.at[k, me], lsem.at[k])

    fetch(0)
    for k in range(chunks):
        local(k).start()
    fetch(1)

    A, B = pl.ds(0, half), pl.ds(half, half)

    def own(k, way, part):
        ref = xg.at[k, me, (A, B)[part]]
        return remote(ref, ref, own_s.at[way, part, k], own_r.at[way, part, k], (right, left)[way])

    def fwd(k, way):
        ref = xg.at[k, (left, right)[way], (A, B)[way]]
        return remote(ref, ref, fwd_s.at[way, k], fwd_r.at[way, k], (right, left)[way])

    def par(k, i):
        ref = (xg.at[k, me], xg.at[k, left], xg.at[k, right], xg.at[k, opp, A], xg.at[k, opp, B])[i]
        return remote(ref, ref, par_s.at[i, k], par_r.at[i, k], partner)

    def send_own(k):
        own(k, 0, 0).start()
        own(k, 1, 1).start()
        own(k, 0, 1).start()
        own(k, 1, 0).start()
        par(k, 0).start()

    rt_all[me] = rt[...]
    greet(n, me)
    local(0).wait()
    send_own(0)
    for off in range(1, n):
        remote(rt, rt_all.at[me], rts.at[off], rtr.at[off], (me + off) % n).start()

    def near(k):
        own(k, 0, 0).wait_recv()
        fwd(k, 0).start()
        own(k, 1, 1).wait_recv()
        fwd(k, 1).start()

        @pl.when(k + 1 < chunks)
        def _():
            send_own(k + 1)

        own(k, 0, 1).wait_recv()
        par(k, 1).start()
        own(k, 1, 0).wait_recv()
        par(k, 2).start()

    def far(k):
        fwd(k, 0).wait_recv()
        par(k, 3).start()
        fwd(k, 1).wait_recv()
        par(k, 4).start()

    def service(g, e):
        @pl.when((e == 4) & (g < chunks))
        def _():
            near(g)

        @pl.when((e == per - 1) & (g < chunks))
        def _():
            far(g)

    def gate_up(e, lhs, slot, first, n_rows):
        width = 2 * ff
        for c in range(0, width, NT):
            cols = pl.ds(c, min(NT, width - c))
            old = acc[e, pl.ds(0, n_rows), cols]
            acc[e, pl.ds(0, n_rows), cols] = jnp.where(first, 0.0, old) + dot(lhs, wbuf[slot, :, cols])

    def act(e, hslot, n_rows):
        step = 32

        @pl.loop(0, n_rows // step)
        def _(r):
            at = pl.ds(pl.multiple_of(r * step, step), step)
            g = acc[e, at, pl.ds(0, ff)]
            u = acc[e, at, pl.ds(ff, ff)]
            hst[hslot, at, :] = (jax.nn.silu(g) * u).astype(BF)

    def shared_out():
        return pltpu.make_async_copy(hst.at[0, pl.ds(0, T)], hs_out, hsem.at[0])

    def expert_out(e):
        return pltpu.make_async_copy(hst.at[e % 2], h_out.at[e], hsem.at[e % 2])

    @pl.loop(0, chunks)
    def _(t):
        arrived(t)
        fetch(t + 2)

        @pl.when(t > 0)
        def _():
            local(t).wait()

        gate_up(0, xg[t, me], t % 3, t == 0, T)
        service(0, t)

    act(0, 0, T)
    shared_out().start()

    for off in range(1, n):
        remote(rt, rt_all.at[me], rts.at[off], rtr.at[off], (me + off) % n).wait()

    @pl.loop(0, n)
    def _(b):
        row = lax.broadcasted_iota(jnp.int32, (mine, T), 0).astype(F32) + (me * mine).astype(F32)
        codes = rt_all[b]
        hit = jnp.zeros((mine, T), F32)
        for j in range(codes.shape[0] // 2):
            hit = jnp.where(codes[j:j + 1, :] == row, 1.0, hit)
        oh[b] = hit.astype(BF)

    @pl.loop(0, chunks)
    def _(k):
        for i in range(5):
            par(k, i).wait_recv()

        @pl.loop(0, n // 2)
        def _(p):
            for i in range(2):
                b = p * 2 + i
                for c in range(0, W, NT):
                    zf[i, :, pl.ds(c, NT)] = dot(oh[b], xg[k, b, :, pl.ds(c, NT)])
            at = pl.ds(pl.multiple_of(p * 2 * slots, 16), 2 * slots)
            for e in range(per):
                lines = pl.ds(e * slots, slots)
                z[e, at, :] = jnp.concatenate([zf[0, lines, :], zf[1, lines, :]], axis=0).astype(BF)

        @pl.loop(0, per)
        def _(e):
            t = chunks + k * per + e
            arrived(t)
            fetch(t + 2)
            gate_up(e, z[e], t % 3, k == 0, rows)
            service(k + 1, e)

            @pl.when(k == chunks - 1)
            def _():
                @pl.when(e == 0)
                def _():
                    shared_out().wait()

                @pl.when(e >= 2)
                def _():
                    expert_out(e - 2).wait()

                act(e, e % 2, rows)
                expert_out(e).start()

    expert_out(per - 2).wait()
    expert_out(per - 1).wait()

    @pl.loop(0, chunks)
    def _(k):
        for way in range(2):
            own(k, way, 0).wait_send()
            own(k, way, 1).wait_send()
            fwd(k, way).wait_send()
        for i in range(5):
            par(k, i).wait_send()


def finish(n, slots, h, hs, rt_all, wd, sd, y,
           hv, hsv, cm, wbuf, of, o, keep, psend, precv, tot, s3, s1s, s1r, s3s, s3r, yb,
           hsem, wsem, ysem, par_s, par_r, s1_s, s1_r, s3_s, s3_r):
    per, ff, D = wd.shape
    T = hs.shape[0]
    half, chunks = T // 2, D // W
    me, chip, core, partner, right, left, opp = places()
    mine = per * slots
    steps = per + 1
    A, B = pl.ds(0, half), pl.ds(half, half)
    parts = (A, B)
    depth = wbuf.shape[0]

    def expert_tile(k, e, slot):
        return pltpu.make_async_copy(wd.at[e, :, pl.ds(k * W, W)], wbuf.at[slot], wsem.at[slot])

    def shared_tile(k, slot):
        return pltpu.make_async_copy(sd.at[:, pl.ds(k * W, W)], wbuf.at[slot], wsem.at[slot])

    def fetch(t):
        slot, k, i = t % depth, t // steps, t % steps

        @pl.when((t < chunks * steps) & (i < per))
        def _():
            expert_tile(k, i, slot).start()

        @pl.when((t < chunks * steps) & (i == per))
        def _():
            shared_tile(k, slot).start()

    def arrived(t):
        shared_tile(0, t % depth).wait()

    def load(e):
        return pltpu.make_async_copy(h.at[e], hv.at[e], hsem.at[e])

    load_s = pltpu.make_async_copy(hs, hsv, hsem.at[per])
    load(0).start()
    fetch(0)
    load(1).start()
    fetch(1)
    for e in range(2, per):
        load(e).start()
    load_s.start()
    for t in range(2, depth - 1):
        fetch(t)

    pad = o.shape[1]

    @pl.loop(0, n)
    def _(b):
        at = lax.broadcasted_iota(jnp.int32, (pad, T), 0)
        row = jnp.where(at < mine, at + me * mine, -2).astype(F32)
        table = rt_all[b]
        top = table.shape[0] // 2
        got = jnp.zeros((pad, T), F32)
        for j in range(top):
            got = jnp.where(table[j:j + 1, :] == row, table[top + j:top + j + 1, :], got)
        cm[b] = got.T.astype(BF)
        o[b, pl.ds(mine, pad - mine), :] = jnp.zeros((pad - mine, W), BF)

    greet(n, me)

    def pair(k):
        return remote(psend.at[k % 2], precv.at[k], par_s.at[k], par_r.at[k], partner)

    def first(k, way):
        return remote(s1s.at[k, way], s1r.at[k, way], s1_s.at[way, k], s1_r.at[way, k], (right, left)[way])

    def second(k, way, part):
        return remote(s3s.at[k, way, parts[part]], s3r.at[k, way, parts[part]],
                      s3_s.at[way, part, k], s3_r.at[way, part, k], (right, left)[way])

    def chip_sums(k):
        pair(k).wait_recv()
        cols = pl.ds(pl.multiple_of(k * W, W), W)

        def both(step, part):
            c = (chip + step) % 4
            return keep[c, parts[part], :] + precv[k, c, parts[part], :].astype(F32)

        for way in range(2):
            s1s[k, way] = both(2, way).astype(BF)
            first(k, way).start()
        for way in range(2):
            far = 1 - way
            s3s[k, way, parts[far], :] = both((1, 3)[way], far).astype(BF)
            second(k, way, far).start()
        for way in range(2):
            s3[k, way] = both((1, 3)[way], way)
        for part in range(2):
            tot[parts[part], cols] = tot[parts[part], cols] + both(0, part)

    def pass_on(k):
        for way in range(2):
            first(k, way).wait_recv()
            s3s[k, way, parts[way], :] = (s3[k, way] + s1r[k, way].astype(F32)).astype(BF)
            second(k, way, way).start()

    def out(k):
        return pltpu.make_async_copy(yb.at[k % 2], y.at[:, pl.ds(k * W, W)], ysem.at[k % 2])

    def complete(k):
        for way in range(2):
            for part in range(2):
                second(k, way, part).wait_recv()

        @pl.when(k >= 2)
        def _():
            out(k - 2).wait()

        cols = pl.ds(pl.multiple_of(k * W, W), W)
        yb[k % 2] = (tot[:, cols] + s3r[k, 0].astype(F32) + s3r[k, 1].astype(F32)).astype(BF)
        out(k).start()

    @pl.loop(0, chunks)
    def _(k):
        @pl.loop(0, per // 2)
        def _(p):
            for i in range(2):
                e = p * 2 + i
                t = k * steps + e
                arrived(t)
                fetch(t + depth - 1)

                @pl.when(k == 0)
                def _():
                    load(e).wait()

                for c in range(0, W, NT):
                    of[i, :, pl.ds(c, NT)] = dot(hv[e], wbuf[t % depth, :, pl.ds(c, NT)])
            at = pl.ds(pl.multiple_of(p * 2 * slots, 16), 2 * slots)
            for b in range(n):
                lines = pl.ds(b * slots, slots)
                o[b, at, :] = jnp.concatenate([of[0, lines, :], of[1, lines, :]], axis=0).astype(BF)

            @pl.when((p == 1) & (k >= 1))
            def _():
                chip_sums(k - 1)

            @pl.when((p == 2) & (k >= 2))
            def _():
                pass_on(k - 2)

            @pl.when((p == 3) & (k >= 4))
            def _():
                complete(k - 4)

        t = k * steps + per
        arrived(t)
        fetch(t + depth - 1)

        @pl.when(k == 0)
        def _():
            load_s.wait()

        @pl.when(k >= 2)
        def _():
            pair(k - 2).wait_send()

        @pl.loop(0, n // 2)
        def _(c):
            psend[k % 2, c] = dot(cm[c * 2 + 1 - core], o[c * 2 + 1 - core]).astype(BF)

        pair(k).start()

        @pl.loop(0, n // 2)
        def _(c):
            keep[c] = dot(cm[c * 2 + core], o[c * 2 + core])

        cols = pl.ds(pl.multiple_of(k * W, W), W)
        tot[:, cols] = dot(hsv[...], wbuf[t % depth])

    chip_sums(chunks - 1)
    pass_on(chunks - 2)
    pass_on(chunks - 1)
    for k in range(chunks - 4, chunks):
        complete(k)
    out(chunks - 2).wait()
    out(chunks - 1).wait()
    for k in range(chunks - 2, chunks):
        pair(k).wait_send()

    @pl.loop(0, chunks)
    def _(k):
        for way in range(2):
            first(k, way).wait_send()
            for part in range(2):
                second(k, way, part).wait_send()


def solution(mesh):
    n = mesh.shape["ep"]

    def body(x, expert, slot, gate, wg, wu, wd, sg, su, sd):
        T, D = x.shape[2:]
        top = expert.shape[3]
        per, _, ff = wg.shape
        slots = 5 * T * top // (4 * per * n)
        rows, chunks = n * slots, D // W
        code = jnp.where(slot < slots, expert * slots + slot, -1).astype(F32)
        rt = jnp.concatenate([code[0, 0].T, gate[0, 0].T], axis=0)
        dma = pltpu.SemaphoreType.DMA
        limit = 67043328
        h, hs, rt_all = pl.pallas_call(
            functools.partial(project, n, slots),
            out_shape=[
                jax.ShapeDtypeStruct((per, rows, ff), BF),
                jax.ShapeDtypeStruct((T, ff), BF),
                jax.ShapeDtypeStruct((n, 2 * top, T), F32),
            ],
            in_specs=[ANY, VM] + [ANY] * 4,
            out_specs=[ANY, ANY, VM],
            scratch_shapes=[
                pltpu.VMEM((chunks, n, T, W), BF),
                pltpu.VMEM((n, per * slots, T), BF),
                pltpu.VMEM((per, rows, 2 * ff), F32),
                pltpu.VMEM((3, W, 2 * ff), BF),
                pltpu.VMEM((2, rows, W), F32),
                pltpu.VMEM((per, rows, W), BF),
                pltpu.VMEM((2, rows, ff), BF),
                dma((chunks,)), dma((3, 2)), dma((2,)),
                dma((n,)), dma((n,)),
                dma((2, 2, chunks)), dma((2, 2, chunks)),
                dma((2, chunks)), dma((2, chunks)),
                dma((5, chunks)), dma((5, chunks)),
            ],
            compiler_params=pltpu.CompilerParams(
                collective_id=0, has_side_effects=True, vmem_limit_bytes=limit),
            name="project",
        )(x[0, 0], rt, sg, su, wg, wu)
        pad = -(-per * slots // 128) * 128
        y = pl.pallas_call(
            functools.partial(finish, n, slots),
            out_shape=jax.ShapeDtypeStruct((T, D), BF),
            in_specs=[ANY, ANY, VM, ANY, ANY],
            out_specs=ANY,
            scratch_shapes=[
                pltpu.VMEM((per, rows, ff), BF),
                pltpu.VMEM((T, ff), BF),
                pltpu.VMEM((n, T, pad), BF),
                pltpu.VMEM((4, ff, W), BF),
                pltpu.VMEM((2, rows, W), F32),
                pltpu.VMEM((n, pad, W), BF),
                pltpu.VMEM((n // 2, T, W), F32),
                pltpu.VMEM((2, n // 2, T, W), BF),
                pltpu.VMEM((chunks, n // 2, T, W), BF),
                pltpu.VMEM((T, D), F32),
                pltpu.VMEM((chunks, 2, T // 2, W), F32),
                pltpu.VMEM((chunks, 2, T // 2, W), BF),
                pltpu.VMEM((chunks, 2, T // 2, W), BF),
                pltpu.VMEM((chunks, 2, T, W), BF),
                pltpu.VMEM((chunks, 2, T, W), BF),
                pltpu.VMEM((2, T, W), BF),
                dma((per + 1,)), dma((4,)), dma((2,)),
                dma((chunks,)), dma((chunks,)),
                dma((2, chunks)), dma((2, chunks)),
                dma((2, 2, chunks)), dma((2, 2, chunks)),
            ],
            compiler_params=pltpu.CompilerParams(
                collective_id=1, has_side_effects=True, vmem_limit_bytes=limit),
            name="finish",
        )(h, hs, rt_all, wd, sd)
        return y[None, None]

    lead = P("dp", "ep", None, None)
    w = P("ep", None, None)
    s = P(None, None)
    return jax.shard_map(
        body, mesh=mesh, in_specs=(lead,) * 4 + (w,) * 3 + (s,) * 3, out_specs=lead, check_vma=False
    )
```

```python
import functools

import jax
import jax.numpy as jnp
from jax import lax
from jax.experimental import pallas as pl
from jax.experimental.pallas import tpu as pltpu
from jax.sharding import PartitionSpec as P

MESH = pl.DeviceIdType.MESH
BF, F32 = jnp.bfloat16, jnp.float32
ANY = pl.BlockSpec(memory_space=pl.ANY)
W = 512
NT = 256


def dot(a, b):
    return jnp.dot(a, b, preferred_element_type=F32)


def silu(v):
    return 0.5 * v * (1.0 + jnp.tanh(0.5 * v))


def remote(src, dst, send, recv, to):
    return pltpu.make_async_remote_copy(
        src_ref=src, dst_ref=dst, send_sem=send, recv_sem=recv,
        device_id={"ep": to}, device_id_type=MESH,
    )


def places():
    me = lax.axis_index("ep")
    chip, core = me // 2, me % 2
    at = lambda step: ((chip + step) % 4) * 2 + core
    return me, chip, core, chip * 2 + 1 - core, at(1), at(3), at(2)


def greet(n, me):
    barrier = pltpu.get_barrier_semaphore()
    for off in range(1, n):
        pl.semaphore_signal(barrier, inc=1, device_id={"ep": (me + off) % n}, device_id_type=MESH)
    pl.semaphore_wait(barrier, n - 1)


def project(n, slots, x, rt, sg, su, wg, wu, h_out, hs_out, rt_out,
            rt_all, xg, oh, acc, wbuf, z, hst, lsem, wsem, hsem, rts, rtr, own_s, own_r, fwd_s, fwd_r, par_s, par_r):
    per, _, ff = wg.shape
    T, D = x.shape
    half, rows, chunks = T // 2, n * slots, D // W
    me, chip, core, partner, right, left, opp = places()
    mine = per * slots

    def tile_copies(g, e, slot):
        return (
            pltpu.make_async_copy(wg.at[e, pl.ds(g * W, W), :], wbuf.at[slot, :, pl.ds(0, ff)], wsem.at[slot, 0]),
            pltpu.make_async_copy(wu.at[e, pl.ds(g * W, W), :], wbuf.at[slot, :, pl.ds(ff, ff)], wsem.at[slot, 1]),
        )

    def shared_copies(g, slot):
        return (
            pltpu.make_async_copy(sg.at[pl.ds(g * W, W), :], wbuf.at[slot, :, pl.ds(0, ff)], wsem.at[slot, 0]),
            pltpu.make_async_copy(su.at[pl.ds(g * W, W), :], wbuf.at[slot, :, pl.ds(ff, ff)], wsem.at[slot, 1]),
        )

    def fetch(t):
        slot = t % 3

        @pl.when(t < chunks)
        def _():
            for c in shared_copies(t, slot):
                c.start()

        @pl.when((t >= chunks) & (t < chunks + chunks * per))
        def _():
            for c in tile_copies((t - chunks) // per, (t - chunks) % per, slot):
                c.start()

    def arrived(t):
        for c in shared_copies(0, t % 3):
            c.wait()

    def local(k):
        return pltpu.make_async_copy(x.at[:, pl.ds(k * W, W)], xg.at[k, me], lsem.at[k])

    fetch(0)
    for k in range(chunks):
        local(k).start()
    fetch(1)

    A, B = pl.ds(0, half), pl.ds(half, half)

    def own(k, way, part):
        ref = xg.at[k, me, (A, B)[part]]
        return remote(ref, ref, own_s.at[way, part, k], own_r.at[way, part, k], (right, left)[way])

    def fwd(k, way):
        ref = xg.at[k, (left, right)[way], (A, B)[way]]
        return remote(ref, ref, fwd_s.at[way, k], fwd_r.at[way, k], (right, left)[way])

    def par(k, i):
        ref = (xg.at[k, me], xg.at[k, left], xg.at[k, right], xg.at[k, opp, A], xg.at[k, opp, B])[i]
        return remote(ref, ref, par_s.at[i, k], par_r.at[i, k], partner)

    def send_own(k):
        own(k, 0, 0).start()
        own(k, 1, 1).start()
        own(k, 0, 1).start()
        own(k, 1, 0).start()
        par(k, 0).start()

    mine_in = pltpu.make_async_copy(rt, rt_all.at[me], rts.at[0])
    mine_in.start()
    greet(n, me)
    local(0).wait()
    send_own(0)
    for off in range(1, n):
        remote(rt, rt_all.at[me], rts.at[off], rtr.at[off], (me + off) % n).start()

    def near(k):
        own(k, 0, 0).wait_recv()
        fwd(k, 0).start()
        own(k, 1, 1).wait_recv()
        fwd(k, 1).start()

        @pl.when(k + 1 < chunks)
        def _():
            send_own(k + 1)

    def across(k):
        own(k, 0, 1).wait_recv()
        par(k, 1).start()
        own(k, 1, 0).wait_recv()
        par(k, 2).start()

    def far(k):
        fwd(k, 0).wait_recv()
        par(k, 3).start()
        fwd(k, 1).wait_recv()
        par(k, 4).start()

    def service(g, e):
        @pl.when(e == 1)
        def _():
            near(g)

        @pl.when(e == 3)
        def _():
            across(g)

        @pl.when(e == per - 2)
        def _():
            far(g)

    def gate_up(e, lhs, slot, first, n_rows):
        width = 2 * ff
        for c in range(0, width, NT):
            cols = pl.ds(c, min(NT, width - c))
            lone = width - c <= NT and (width // NT) % 2 == 1
            step = n_rows // 2 if lone else n_rows
            for r in range(0, n_rows, step):
                at = pl.ds(r, step)
                part = dot(lhs[r:r + step], wbuf[slot, :, cols])
                acc[e, at, cols] = jnp.where(first, 0.0, acc[e, at, cols]) + part

    def gate_up_act(e, lhs, slot, hslot, n_rows):
        at = pl.ds(0, n_rows)
        for c in range(0, ff, NT):
            g_cols = pl.ds(c, min(NT, ff - c))
            u_cols = pl.ds(ff + c, min(NT, ff - c))
            g = acc[e, at, g_cols] + dot(lhs, wbuf[slot, :, g_cols])
            u = acc[e, at, u_cols] + dot(lhs, wbuf[slot, :, u_cols])
            hst[hslot, at, g_cols] = (silu(g) * u).astype(BF)

    def shared_out():
        return pltpu.make_async_copy(hst.at[0, pl.ds(0, T)], hs_out, hsem.at[0])

    def expert_out(e):
        return pltpu.make_async_copy(hst.at[e % 2], h_out.at[e], hsem.at[e % 2])

    @pl.loop(0, chunks - 1)
    def _(t):
        arrived(t)
        fetch(t + 2)

        @pl.when(t > 0)
        def _():
            local(t).wait()

        gate_up(0, xg[t, me], t % 3, t == 0, T)

        @pl.when(t == 3)
        def _():
            near(0)

    last = chunks - 1
    arrived(last)
    fetch(last + 2)
    local(last).wait()
    gate_up_act(0, xg[last, me], last % 3, 0, T)
    across(0)
    shared_out().start()

    for off in range(1, n):
        remote(rt, rt_all.at[me], rts.at[off], rtr.at[off], (me + off) % n).wait()
    mine_in.wait()
    tables = pltpu.make_async_copy(rt_all, rt_out, rts.at[0])
    tables.start()

    @pl.loop(0, n)
    def _(b):
        row = lax.broadcasted_iota(jnp.int32, (mine, T), 0).astype(F32) + (me * mine).astype(F32)
        codes = rt_all[b]
        hit = jnp.zeros((mine, T), F32)
        for j in range(codes.shape[0] // 2):
            hit = jnp.where(codes[j:j + 1, :] == row, 1.0, hit)
        oh[b] = hit.astype(BF)

    far(0)

    def dispatch(k):
        for i in range(5):
            par(k, i).wait_recv()
        for p in range(n // 2):
            at = pl.ds(p * 2 * slots, 2 * slots)
            for c in range(0, W, NT):
                cols = pl.ds(c, NT)
                two = [dot(oh[b], xg[k, b, :, cols]) for b in (p * 2, p * 2 + 1)]
                for e in range(per):
                    z[e, at, cols] = jnp.concatenate([v[e * slots:(e + 1) * slots] for v in two], axis=0).astype(BF)

    @pl.loop(0, last)
    def _(k):
        dispatch(k)

        @pl.loop(0, per)
        def _(e):
            t = chunks + k * per + e
            arrived(t)
            fetch(t + 2)
            service(k + 1, e)
            gate_up(e, z[e], t % 3, k == 0, rows)

    dispatch(last)
    shared_out().wait()

    @pl.loop(0, per)
    def _(e):
        t = chunks + last * per + e
        arrived(t)
        fetch(t + 2)

        @pl.when(e >= 2)
        def _():
            expert_out(e - 2).wait()

        gate_up_act(e, z[e], t % 3, e % 2, rows)
        expert_out(e).start()

    tables.wait()
    expert_out(per - 2).wait()
    expert_out(per - 1).wait()

    @pl.loop(0, chunks)
    def _(k):
        for way in range(2):
            own(k, way, 0).wait_send()
            own(k, way, 1).wait_send()
            fwd(k, way).wait_send()
        for i in range(5):
            par(k, i).wait_send()


def finish(n, slots, h, hs, rt_in, wd, sd, y,
           rt_all, hv, hsv, cm, wbuf, o, keep, psend, precv, tot, s3, s1s, s1r, s3s, s3r, yb,
           hsem, wsem, ysem, par_s, par_r, s1_s, s1_r, s3_s, s3_r):
    per, ff, D = wd.shape
    T = hs.shape[0]
    half, chunks = T // 2, D // W
    me, chip, core, partner, right, left, opp = places()
    mine = per * slots
    steps = per + 1
    A, B = pl.ds(0, half), pl.ds(half, half)
    parts = (A, B)
    depth = wbuf.shape[0]

    def expert_tile(k, e, slot):
        return pltpu.make_async_copy(wd.at[e, :, pl.ds(k * W, W)], wbuf.at[slot], wsem.at[slot])

    def shared_tile(k, slot):
        return pltpu.make_async_copy(sd.at[:, pl.ds(k * W, W)], wbuf.at[slot], wsem.at[slot])

    def fetch(t):
        slot, k, i = t % depth, t // steps, t % steps

        @pl.when((t < chunks * steps) & (i < per))
        def _():
            expert_tile(k, i, slot).start()

        @pl.when((t < chunks * steps) & (i == per))
        def _():
            shared_tile(k, slot).start()

    def arrived(t):
        shared_tile(0, t % depth).wait()

    def load(e):
        return pltpu.make_async_copy(h.at[e], hv.at[e], hsem.at[e])

    load_s = pltpu.make_async_copy(hs, hsv, hsem.at[per])
    tables = pltpu.make_async_copy(rt_in, rt_all, hsem.at[per + 1])
    tables.start()
    load(0).start()
    fetch(0)
    load(1).start()
    fetch(1)
    for e in range(2, per):
        load(e).start()
    load_s.start()
    for t in range(2, 4):
        fetch(t)

    pad = o.shape[1]
    tables.wait()

    @pl.loop(0, n)
    def _(b):
        at = lax.broadcasted_iota(jnp.int32, (pad, T), 0)
        row = jnp.where(at < mine, at + me * mine, -2).astype(F32)
        table = rt_all[b]
        top = table.shape[0] // 2
        got = jnp.zeros((pad, T), F32)
        for j in range(top):
            got = jnp.where(table[j:j + 1, :] == row, table[top + j:top + j + 1, :], got)
        cm[b] = got.T.astype(BF)
        o[b, pl.ds(mine, pad - mine), :] = jnp.zeros((pad - mine, W), BF)

    greet(n, me)

    def pair(k):
        return remote(psend.at[k % 2], precv.at[k], par_s.at[k], par_r.at[k], partner)

    def first(k, way):
        return remote(s1s.at[k, way], s1r.at[k, way], s1_s.at[way, k], s1_r.at[way, k], (right, left)[way])

    def second(k, way, part):
        return remote(s3s.at[k, way, parts[part]], s3r.at[k, way, parts[part]],
                      s3_s.at[way, part, k], s3_r.at[way, part, k], (right, left)[way])

    def chip_sums(k):
        pair(k).wait_recv()
        cols = pl.ds(pl.multiple_of(k * W, W), W)

        def both(step, part):
            c = (chip + step) % 4
            return keep[c, parts[part], :] + precv[k, c, parts[part], :].astype(F32)

        for way in range(2):
            s1s[k, way] = both(2, way).astype(BF)
            first(k, way).start()
        for way in range(2):
            far = 1 - way
            s3s[k, way, parts[far], :] = both((1, 3)[way], far).astype(BF)
            second(k, way, far).start()
        for way in range(2):
            s3[k, way] = both((1, 3)[way], way)
        for part in range(2):
            tot[parts[part], cols] = tot[parts[part], cols] + both(0, part)

    def pass_on(k):
        for way in range(2):
            first(k, way).wait_recv()
            s3s[k, way, parts[way], :] = (s3[k, way] + s1r[k, way].astype(F32)).astype(BF)
            second(k, way, way).start()

    def out(k):
        return pltpu.make_async_copy(yb.at[k % 2], y.at[:, pl.ds(k * W, W)], ysem.at[k % 2])

    def complete(k):
        for way in range(2):
            for part in range(2):
                second(k, way, part).wait_recv()

        @pl.when(k >= 2)
        def _():
            out(k - 2).wait()

        cols = pl.ds(pl.multiple_of(k * W, W), W)
        yb[k % 2] = (tot[:, cols] + s3r[k, 0].astype(F32) + s3r[k, 1].astype(F32)).astype(BF)
        out(k).start()

    @pl.loop(0, chunks)
    def _(k):
        @pl.loop(0, per // 2)
        def _(p):
            t = k * steps + p * 2
            for i in range(2):
                arrived(t + i)
                fetch(t + 4 + i)

                @pl.when(k == 0)
                def _():
                    load(p * 2 + i).wait()

            at = pl.ds(pl.multiple_of(p * 2 * slots, 16), 2 * slots)
            for c in range(0, W, NT):
                cols = pl.ds(c, NT)
                two = [dot(hv[p * 2 + i], wbuf[(t + i) % depth, :, cols]) for i in range(2)]
                for b in range(n):
                    o[b, at, cols] = jnp.concatenate([v[b * slots:(b + 1) * slots] for v in two], axis=0).astype(BF)

            @pl.when((p == 0) & (k >= 1))
            def _():
                chip_sums(k - 1)

            @pl.when((p == 1) & (k >= 2))
            def _():
                pass_on(k - 2)

            @pl.when((p == 2) & (k >= 4))
            def _():
                complete(k - 4)

        t = k * steps + per
        arrived(t)
        fetch(t + 4)

        @pl.when(k == 0)
        def _():
            load_s.wait()

        @pl.when(k >= 2)
        def _():
            pair(k - 2).wait_send()

        for c in range(n // 2):
            b = c * 2 + 1 - core
            psend[k % 2, c] = dot(cm[b], o[b]).astype(BF)
        pair(k).start()
        for c in range(n // 2):
            b = c * 2 + core
            keep[c] = dot(cm[b], o[b])
        cols = pl.ds(pl.multiple_of(k * W, W), W)
        tot[:, cols] = dot(hsv[...], wbuf[t % depth])

    chip_sums(chunks - 1)
    pass_on(chunks - 2)
    pass_on(chunks - 1)
    for k in range(chunks - 4, chunks):
        complete(k)
    out(chunks - 2).wait()
    out(chunks - 1).wait()
    for k in range(chunks - 2, chunks):
        pair(k).wait_send()

    @pl.loop(0, chunks)
    def _(k):
        for way in range(2):
            first(k, way).wait_send()
            for part in range(2):
                second(k, way, part).wait_send()


def solution(mesh):
    n = mesh.shape["ep"]

    def body(x, expert, slot, gate, wg, wu, wd, sg, su, sd):
        T, D = x.shape[2:]
        top = expert.shape[3]
        per, _, ff = wg.shape
        slots = 5 * T * top // (4 * per * n)
        rows, chunks = n * slots, D // W
        code = jnp.where(slot < slots, expert * slots + slot, -1).astype(F32)
        rt = jnp.concatenate([code[0, 0].T, gate[0, 0].T], axis=0)
        dma = pltpu.SemaphoreType.DMA
        limit = 67043328
        h, hs, rt_all = pl.pallas_call(
            functools.partial(project, n, slots),
            out_shape=[
                jax.ShapeDtypeStruct((per, rows, ff), BF),
                jax.ShapeDtypeStruct((T, ff), BF),
                jax.ShapeDtypeStruct((n, 2 * top, T), F32),
            ],
            in_specs=[ANY] * 6,
            out_specs=[ANY] * 3,
            scratch_shapes=[
                pltpu.VMEM((n, 2 * top, T), F32),
                pltpu.VMEM((chunks, n, T, W), BF),
                pltpu.VMEM((n, per * slots, T), BF),
                pltpu.VMEM((per, rows, 2 * ff), F32),
                pltpu.VMEM((3, W, 2 * ff), BF),
                pltpu.VMEM((per, rows, W), BF),
                pltpu.VMEM((2, rows, ff), BF),
                dma((chunks,)), dma((3, 2)), dma((2,)),
                dma((n,)), dma((n,)),
                dma((2, 2, chunks)), dma((2, 2, chunks)),
                dma((2, chunks)), dma((2, chunks)),
                dma((5, chunks)), dma((5, chunks)),
            ],
            compiler_params=pltpu.CompilerParams(
                collective_id=0, has_side_effects=True, vmem_limit_bytes=limit),
            name="project",
        )(x[0, 0], rt, sg, su, wg, wu)
        pad = -(-per * slots // 128) * 128
        y = pl.pallas_call(
            functools.partial(finish, n, slots),
            out_shape=jax.ShapeDtypeStruct((T, D), BF),
            in_specs=[ANY] * 5,
            out_specs=ANY,
            scratch_shapes=[
                pltpu.VMEM((n, 2 * top, T), F32),
                pltpu.VMEM((per, rows, ff), BF),
                pltpu.VMEM((T, ff), BF),
                pltpu.VMEM((n, T, pad), BF),
                pltpu.VMEM((6, ff, W), BF),
                pltpu.VMEM((n, pad, W), BF),
                pltpu.VMEM((n // 2, T, W), F32),
                pltpu.VMEM((2, n // 2, T, W), BF),
                pltpu.VMEM((chunks, n // 2, T, W), BF),
                pltpu.VMEM((T, D), F32),
                pltpu.VMEM((chunks, 2, T // 2, W), F32),
                pltpu.VMEM((chunks, 2, T // 2, W), BF),
                pltpu.VMEM((chunks, 2, T // 2, W), BF),
                pltpu.VMEM((chunks, 2, T, W), BF),
                pltpu.VMEM((chunks, 2, T, W), BF),
                pltpu.VMEM((2, T, W), BF),
                dma((per + 2,)), dma((6,)), dma((2,)),
                dma((chunks,)), dma((chunks,)),
                dma((2, chunks)), dma((2, chunks)),
                dma((2, 2, chunks)), dma((2, 2, chunks)),
            ],
            compiler_params=pltpu.CompilerParams(
                collective_id=1, has_side_effects=True, vmem_limit_bytes=limit),
            name="finish",
        )(h, hs, rt_all, wd, sd)
        return y[None, None]

    lead = P("dp", "ep", None, None)
    w = P("ep", None, None)
    s = P(None, None)
    return jax.shard_map(
        body, mesh=mesh, in_specs=(lead,) * 4 + (w,) * 3 + (s,) * 3, out_specs=lead, check_vma=False
    )
```

```python
import functools

import jax
import jax.numpy as jnp
from jax import lax
from jax.experimental import pallas as pl
from jax.experimental.pallas import tpu as pltpu
from jax.sharding import PartitionSpec as P

MESH = pl.DeviceIdType.MESH
BF, F32 = jnp.bfloat16, jnp.float32
ANY = pl.BlockSpec(memory_space=pl.ANY)
W = 512
NT = 256


def dot(a, b):
    return jnp.dot(a, b, preferred_element_type=F32)


def silu(v):
    return 0.5 * v * (1.0 + jnp.tanh(0.5 * v))


def remote(src, dst, send, recv, to):
    return pltpu.make_async_remote_copy(
        src_ref=src, dst_ref=dst, send_sem=send, recv_sem=recv,
        device_id={"ep": to}, device_id_type=MESH,
    )


def places():
    me = lax.axis_index("ep")
    chip, core = me // 2, me % 2
    at = lambda step: ((chip + step) % 4) * 2 + core
    return me, chip, core, chip * 2 + 1 - core, at(1), at(3), at(2)


def greet(n, me):
    barrier = pltpu.get_barrier_semaphore()
    for off in range(1, n):
        pl.semaphore_signal(barrier, inc=1, device_id={"ep": (me + off) % n}, device_id_type=MESH)
    pl.semaphore_wait(barrier, n - 1)


def project(n, slots, x, rt, sg, su, wg, wu, h_out, hs_out, rt_out,
            rt_all, xg, oh, acc, wbuf, z, hst, lsem, wsem, hsem, rts, rtr, own_s, own_r, fwd_s, fwd_r, par_s, par_r):
    per, _, ff = wg.shape
    T, D = x.shape
    half, rows, chunks = T // 2, n * slots, D // W
    me, chip, core, partner, right, left, opp = places()
    mine = per * slots

    def tile_copies(g, e, slot):
        return (
            pltpu.make_async_copy(wg.at[e, pl.ds(g * W, W), :], wbuf.at[slot, :, pl.ds(0, ff)], wsem.at[slot, 0]),
            pltpu.make_async_copy(wu.at[e, pl.ds(g * W, W), :], wbuf.at[slot, :, pl.ds(ff, ff)], wsem.at[slot, 1]),
        )

    def shared_copies(g, slot):
        return (
            pltpu.make_async_copy(sg.at[pl.ds(g * W, W), :], wbuf.at[slot, :, pl.ds(0, ff)], wsem.at[slot, 0]),
            pltpu.make_async_copy(su.at[pl.ds(g * W, W), :], wbuf.at[slot, :, pl.ds(ff, ff)], wsem.at[slot, 1]),
        )

    def fetch(t):
        slot = t % 3

        @pl.when(t < chunks)
        def _():
            for c in shared_copies(t, slot):
                c.start()

        @pl.when((t >= chunks) & (t < chunks + chunks * per))
        def _():
            for c in tile_copies((t - chunks) // per, (t - chunks) % per, slot):
                c.start()

    def arrived(t):
        for c in shared_copies(0, t % 3):
            c.wait()

    def local(k):
        return pltpu.make_async_copy(x.at[:, pl.ds(k * W, W)], xg.at[k, me], lsem.at[k])

    fetch(0)
    for k in range(chunks):
        local(k).start()
    fetch(1)

    A, B = pl.ds(0, half), pl.ds(half, half)

    def own(k, way, part):
        ref = xg.at[k, me, (A, B)[part]]
        return remote(ref, ref, own_s.at[way, part, k], own_r.at[way, part, k], (right, left)[way])

    def fwd(k, way):
        ref = xg.at[k, (left, right)[way], (A, B)[way]]
        return remote(ref, ref, fwd_s.at[way, k], fwd_r.at[way, k], (right, left)[way])

    def par(k, i):
        ref = (xg.at[k, me], xg.at[k, left], xg.at[k, right], xg.at[k, opp, A], xg.at[k, opp, B])[i]
        return remote(ref, ref, par_s.at[i, k], par_r.at[i, k], partner)

    def send_own(k):
        own(k, 0, 0).start()
        own(k, 1, 1).start()
        own(k, 0, 1).start()
        own(k, 1, 0).start()
        par(k, 0).start()

    mine_in = pltpu.make_async_copy(rt, rt_all.at[me], rts.at[0])
    mine_in.start()
    greet(n, me)
    local(0).wait()
    send_own(0)
    for off in range(1, n):
        remote(rt, rt_all.at[me], rts.at[off], rtr.at[off], (me + off) % n).start()

    def near(k):
        own(k, 0, 0).wait_recv()
        fwd(k, 0).start()
        own(k, 1, 1).wait_recv()
        fwd(k, 1).start()

        @pl.when(k + 1 < chunks)
        def _():
            send_own(k + 1)

    def across(k):
        own(k, 0, 1).wait_recv()
        par(k, 1).start()
        own(k, 1, 0).wait_recv()
        par(k, 2).start()

    def far(k):
        fwd(k, 0).wait_recv()
        par(k, 3).start()
        fwd(k, 1).wait_recv()
        par(k, 4).start()

    def service(g, e):
        @pl.when(e == 1)
        def _():
            near(g)

        @pl.when(e == 3)
        def _():
            across(g)

        @pl.when(e == per - 2)
        def _():
            far(g)

    def gate_up(e, lhs, slot, first, n_rows):
        width = 2 * ff
        for c in range(0, width, NT):
            cols = pl.ds(c, min(NT, width - c))
            lone = width - c <= NT and (width // NT) % 2 == 1
            step = n_rows // 2 if lone else n_rows
            for r in range(0, n_rows, step):
                at = pl.ds(r, step)
                part = dot(lhs[r:r + step], wbuf[slot, :, cols])
                acc[e, at, cols] = jnp.where(first, 0.0, acc[e, at, cols]) + part

    def gate_up_act(e, lhs, slot, hslot, n_rows):
        at = pl.ds(0, n_rows)
        for c in range(0, ff, NT):
            g_cols = pl.ds(c, min(NT, ff - c))
            u_cols = pl.ds(ff + c, min(NT, ff - c))
            g = acc[e, at, g_cols] + dot(lhs, wbuf[slot, :, g_cols])
            u = acc[e, at, u_cols] + dot(lhs, wbuf[slot, :, u_cols])
            hst[hslot, at, g_cols] = (silu(g) * u).astype(BF)

    def shared_out():
        return pltpu.make_async_copy(hst.at[0, pl.ds(0, T)], hs_out, hsem.at[0])

    def expert_out(e):
        return pltpu.make_async_copy(hst.at[e % 2], h_out.at[e], hsem.at[e % 2])

    @pl.loop(0, chunks - 1)
    def _(t):
        arrived(t)
        fetch(t + 2)

        @pl.when(t > 0)
        def _():
            local(t).wait()

        gate_up(0, xg[t, me], t % 3, t == 0, T)

        @pl.when(t == 3)
        def _():
            near(0)

    last = chunks - 1
    arrived(last)
    fetch(last + 2)
    local(last).wait()
    gate_up_act(0, xg[last, me], last % 3, 0, T)
    across(0)
    shared_out().start()

    for off in range(1, n):
        remote(rt, rt_all.at[me], rts.at[off], rtr.at[off], (me + off) % n).wait()
    mine_in.wait()
    tables = pltpu.make_async_copy(rt_all, rt_out, rts.at[0])
    tables.start()

    @pl.loop(0, n)
    def _(b):
        row = lax.broadcasted_iota(jnp.int32, (mine, T), 0).astype(F32) + (me * mine).astype(F32)
        codes = rt_all[b]
        hit = jnp.zeros((mine, T), F32)
        for j in range(codes.shape[0] // 2):
            hit = jnp.where(codes[j:j + 1, :] == row, 1.0, hit)
        oh[b] = hit.astype(BF)

    far(0)

    def dispatch(k):
        for i in range(5):
            par(k, i).wait_recv()
        for p in range(n // 2):
            at = pl.ds(p * 2 * slots, 2 * slots)
            for c in range(0, W, NT):
                cols = pl.ds(c, NT)
                two = [dot(oh[b], xg[k, b, :, cols]) for b in (p * 2, p * 2 + 1)]
                for e in range(per):
                    z[e, at, cols] = jnp.concatenate([v[e * slots:(e + 1) * slots] for v in two], axis=0).astype(BF)

    @pl.loop(0, last)
    def _(k):
        dispatch(k)

        @pl.loop(0, per)
        def _(e):
            t = chunks + k * per + e
            arrived(t)
            fetch(t + 2)
            service(k + 1, e)
            gate_up(e, z[e], t % 3, k == 0, rows)

    dispatch(last)
    shared_out().wait()

    @pl.loop(0, per)
    def _(e):
        t = chunks + last * per + e
        arrived(t)
        fetch(t + 2)

        @pl.when(e >= 2)
        def _():
            expert_out(e - 2).wait()

        gate_up_act(e, z[e], t % 3, e % 2, rows)
        expert_out(e).start()

    tables.wait()
    expert_out(per - 2).wait()
    expert_out(per - 1).wait()

    @pl.loop(0, chunks)
    def _(k):
        for way in range(2):
            own(k, way, 0).wait_send()
            own(k, way, 1).wait_send()
            fwd(k, way).wait_send()
        for i in range(5):
            par(k, i).wait_send()


def finish(n, slots, h, hs, rt_in, wd, sd, y,
           rt_all, hv, hsv, cm, wbuf, o, keep, psend, precv, tot, s3, s1s, s1r, s3s, s3r, yb,
           hsem, wsem, ysem, par_s, par_r, s1_s, s1_r, s3_s, s3_r):
    per, ff, D = wd.shape
    T = hs.shape[0]
    half, chunks = T // 2, D // W
    me, chip, core, partner, right, left, opp = places()
    mine = per * slots
    steps = per + 1
    A, B = pl.ds(0, half), pl.ds(half, half)
    parts = (A, B)
    depth = wbuf.shape[0]

    def expert_tile(k, e, slot):
        return pltpu.make_async_copy(wd.at[e, :, pl.ds(k * W, W)], wbuf.at[slot], wsem.at[slot])

    def shared_tile(k, slot):
        return pltpu.make_async_copy(sd.at[:, pl.ds(k * W, W)], wbuf.at[slot], wsem.at[slot])

    def fetch(t):
        slot, k, i = t % depth, t // steps, t % steps

        @pl.when((t < chunks * steps) & (i < per))
        def _():
            expert_tile(k, i, slot).start()

        @pl.when((t < chunks * steps) & (i == per))
        def _():
            shared_tile(k, slot).start()

    def arrived(t):
        shared_tile(0, t % depth).wait()

    def load(e):
        return pltpu.make_async_copy(h.at[e], hv.at[e], hsem.at[e])

    load_s = pltpu.make_async_copy(hs, hsv, hsem.at[per])
    tables = pltpu.make_async_copy(rt_in, rt_all, hsem.at[per + 1])
    tables.start()
    load(0).start()
    fetch(0)
    load(1).start()
    fetch(1)
    for e in range(2, per):
        load(e).start()
    load_s.start()
    for t in range(2, 4):
        fetch(t)

    pad = o.shape[1]
    tables.wait()

    @pl.loop(0, n)
    def _(b):
        at = lax.broadcasted_iota(jnp.int32, (pad, T), 0)
        row = jnp.where(at < mine, at + me * mine, -2).astype(F32)
        table = rt_all[b]
        top = table.shape[0] // 2
        got = jnp.zeros((pad, T), F32)
        for j in range(top):
            got = jnp.where(table[j:j + 1, :] == row, table[top + j:top + j + 1, :], got)
        cm[b] = got.T.astype(BF)
        o[b, pl.ds(mine, pad - mine), :] = jnp.zeros((pad - mine, W), BF)

    greet(n, me)

    def pair(k):
        return remote(psend.at[k % 2], precv.at[k], par_s.at[k], par_r.at[k], partner)

    def first(k, way):
        return remote(s1s.at[k, way], s1r.at[k, way], s1_s.at[way, k], s1_r.at[way, k], (right, left)[way])

    def second(k, way):
        return remote(s3s.at[k, way], s3r.at[k, way], s3_s.at[way, k], s3_r.at[way, k], (right, left)[way])

    def chip_sums(k):
        pair(k).wait_recv()
        cols = pl.ds(pl.multiple_of(k * W, W), W)

        def both(step, part):
            c = (chip + step) % 4
            return keep[c, parts[part], :] + precv[k, c, parts[part], :].astype(F32)

        for way in range(2):
            s1s[k, way, 0] = both(2, way).astype(BF)
            s1s[k, way, 1] = both((1, 3)[way], 1 - way).astype(BF)
            first(k, way).start()
        for way in range(2):
            s3[k, way] = both((1, 3)[way], way)
        for part in range(2):
            tot[parts[part], cols] = tot[parts[part], cols] + both(0, part)

    def pass_on(k):
        for way in range(2):
            first(k, way).wait_recv()
            s3s[k, way] = (s3[k, way] + s1r[k, way, 0].astype(F32)).astype(BF)
            second(k, way).start()

    def out(k):
        return pltpu.make_async_copy(yb.at[k % 2], y.at[:, pl.ds(k * W, W)], ysem.at[k % 2])

    def complete(k):
        for way in range(2):
            second(k, way).wait_recv()

        @pl.when(k >= 2)
        def _():
            out(k - 2).wait()

        cols = pl.ds(pl.multiple_of(k * W, W), W)
        for way in range(2):
            sums = tot[parts[way], cols] + s3r[k, way].astype(F32)
            yb[k % 2, parts[way], :] = (sums + s1r[k, 1 - way, 1].astype(F32)).astype(BF)
        out(k).start()

    @pl.loop(0, chunks)
    def _(k):
        @pl.loop(0, per // 2)
        def _(p):
            t = k * steps + p * 2
            for i in range(2):
                arrived(t + i)
                fetch(t + 4 + i)

                @pl.when(k == 0)
                def _():
                    load(p * 2 + i).wait()

            at = pl.ds(pl.multiple_of(p * 2 * slots, 16), 2 * slots)
            for c in range(0, W, NT):
                cols = pl.ds(c, NT)
                two = [dot(hv[p * 2 + i], wbuf[(t + i) % depth, :, cols]) for i in range(2)]
                for b in range(n):
                    o[b, at, cols] = jnp.concatenate([v[b * slots:(b + 1) * slots] for v in two], axis=0).astype(BF)

            @pl.when((p == 0) & (k >= 1))
            def _():
                chip_sums(k - 1)

            @pl.when((p == 1) & (k >= 2))
            def _():
                pass_on(k - 2)

            @pl.when((p == 2) & (k >= 4))
            def _():
                complete(k - 4)

        t = k * steps + per
        arrived(t)
        fetch(t + 4)

        @pl.when(k == 0)
        def _():
            load_s.wait()

        @pl.when(k >= 2)
        def _():
            pair(k - 2).wait_send()

        for c in range(n // 2):
            b = c * 2 + 1 - core
            psend[k % 2, c] = dot(cm[b], o[b]).astype(BF)
        pair(k).start()
        for c in range(n // 2):
            b = c * 2 + core
            keep[c] = dot(cm[b], o[b])
        cols = pl.ds(pl.multiple_of(k * W, W), W)
        tot[:, cols] = dot(hsv[...], wbuf[t % depth])

    chip_sums(chunks - 1)
    pass_on(chunks - 2)
    pass_on(chunks - 1)
    for k in range(chunks - 4, chunks):
        complete(k)
    out(chunks - 2).wait()
    out(chunks - 1).wait()
    for k in range(chunks - 2, chunks):
        pair(k).wait_send()

    @pl.loop(0, chunks)
    def _(k):
        for way in range(2):
            first(k, way).wait_send()
            second(k, way).wait_send()


def solution(mesh):
    n = mesh.shape["ep"]

    def body(x, expert, slot, gate, wg, wu, wd, sg, su, sd):
        T, D = x.shape[2:]
        top = expert.shape[3]
        per, _, ff = wg.shape
        slots = 5 * T * top // (4 * per * n)
        rows, chunks = n * slots, D // W
        code = jnp.where(slot < slots, expert * slots + slot, -1).astype(F32)
        rt = jnp.concatenate([code[0, 0].T, gate[0, 0].T], axis=0)
        dma = pltpu.SemaphoreType.DMA
        limit = 67043328
        h, hs, rt_all = pl.pallas_call(
            functools.partial(project, n, slots),
            out_shape=[
                jax.ShapeDtypeStruct((per, rows, ff), BF),
                jax.ShapeDtypeStruct((T, ff), BF),
                jax.ShapeDtypeStruct((n, 2 * top, T), F32),
            ],
            in_specs=[ANY] * 6,
            out_specs=[ANY] * 3,
            scratch_shapes=[
                pltpu.VMEM((n, 2 * top, T), F32),
                pltpu.VMEM((chunks, n, T, W), BF),
                pltpu.VMEM((n, per * slots, T), BF),
                pltpu.VMEM((per, rows, 2 * ff), F32),
                pltpu.VMEM((3, W, 2 * ff), BF),
                pltpu.VMEM((per, rows, W), BF),
                pltpu.VMEM((2, rows, ff), BF),
                dma((chunks,)), dma((3, 2)), dma((2,)),
                dma((n,)), dma((n,)),
                dma((2, 2, chunks)), dma((2, 2, chunks)),
                dma((2, chunks)), dma((2, chunks)),
                dma((5, chunks)), dma((5, chunks)),
            ],
            compiler_params=pltpu.CompilerParams(
                collective_id=0, has_side_effects=True, vmem_limit_bytes=limit),
            name="project",
        )(x[0, 0], rt, sg, su, wg, wu)
        pad = -(-per * slots // 128) * 128
        y = pl.pallas_call(
            functools.partial(finish, n, slots),
            out_shape=jax.ShapeDtypeStruct((T, D), BF),
            in_specs=[ANY] * 5,
            out_specs=ANY,
            scratch_shapes=[
                pltpu.VMEM((n, 2 * top, T), F32),
                pltpu.VMEM((per, rows, ff), BF),
                pltpu.VMEM((T, ff), BF),
                pltpu.VMEM((n, T, pad), BF),
                pltpu.VMEM((6, ff, W), BF),
                pltpu.VMEM((n, pad, W), BF),
                pltpu.VMEM((n // 2, T, W), F32),
                pltpu.VMEM((2, n // 2, T, W), BF),
                pltpu.VMEM((chunks, n // 2, T, W), BF),
                pltpu.VMEM((T, D), F32),
                pltpu.VMEM((chunks, 2, T // 2, W), F32),
                pltpu.VMEM((chunks, 2, 2, T // 2, W), BF),
                pltpu.VMEM((chunks, 2, 2, T // 2, W), BF),
                pltpu.VMEM((chunks, 2, T // 2, W), BF),
                pltpu.VMEM((chunks, 2, T // 2, W), BF),
                pltpu.VMEM((2, T, W), BF),
                dma((per + 2,)), dma((6,)), dma((2,)),
                dma((chunks,)), dma((chunks,)),
                dma((2, chunks)), dma((2, chunks)),
                dma((2, chunks)), dma((2, chunks)),
            ],
            compiler_params=pltpu.CompilerParams(
                collective_id=1, has_side_effects=True, vmem_limit_bytes=limit),
            name="finish",
        )(h, hs, rt_all, wd, sd)
        return y[None, None]

    lead = P("dp", "ep", None, None)
    w = P("ep", None, None)
    s = P(None, None)
    return jax.shard_map(
        body, mesh=mesh, in_specs=(lead,) * 4 + (w,) * 3 + (s,) * 3, out_specs=lead, check_vma=False
    )
```
